32 devices in a mesh: dp: 16 (over z, y, x), mp: 2 (over core).
Axes of the slice: x: 2, y: 2, z: 4, core: 2. Of those that a mesh axis runs over, the one named last changes fastest.
Arguments:
- frames: float32 [8192, 768], P('dp'), may hold values from -6 to 6
- clip_ids: int32 [8192], replicated, may hold values from 0 to 8, never falling along the last dimension, each value on 1 to 1500 neighbouring positions
- first_gain: float32 [768], replicated, may hold values from 0.5 to 1.5
- first_shift: float32 [768], replicated, may hold values from -1.75 to 1.75
- input_weight: float32 [768, 3, 768], P(None, None, 'mp'), may hold values from -1.5 to 1.5
- input_bias: float32 [2, 768], P(None, 'mp'), may hold values from -1.75 to 1.75
- output_weight: float32 [768, 768], P('mp'), may hold values from -1.25 to 1.25
- output_bias: float32 [768], replicated, may hold values from -1.75 to 1.75
- second_gain: float32 [768], replicated, may hold values from 0.5 to 1.5
- second_shift: float32 [768], replicated, may hold values from -1.75 to 1.75
- expand_weight: float32 [768, 3072], P(None, 'mp'), may hold values from -0.21875 to 0.21875
- expand_bias: float32 [3072], P('mp'), may hold values from -3 to 3
- contract_weight: float32 [3072, 768], P('mp'), may hold values from -0.109375 to 0.109375
- contract_bias: float32 [768], replicated, may hold values from -1.75 to 1.75
- cotangent: float32 [8192, 768], P('dp'), may hold values from -6 to 6
Outputs:
- block_output: float32 [8192, 768], P('dp')
- grad_frames: float32 [8192, 768], P('dp')
- grad_first_gain: float32 [768], replicated
- grad_first_shift: float32 [768], replicated
- grad_input_weight: float32 [768, 3, 768], P(None, None, 'mp')
- grad_input_bias: float32 [2, 768], P(None, 'mp')
- grad_output_weight: float32 [768, 768], P('mp')
- grad_output_bias: float32 [768], replicated
- grad_second_gain: float32 [768], replicated
- grad_second_shift: float32 [768], replicated
- grad_expand_weight: float32 [768, 3072], P(None, 'mp')
- grad_expand_bias: float32 [3072], P('mp')
- grad_contract_weight: float32 [3072, 768], P('mp')
- grad_contract_bias: float32 [768], replicated
The draws below stay inside these ranges and needn't reach their ends.
Inputs may be any that keep to these rules, and one draw needn't show every extreme that they name: `clip_ids`: clip numbers never fall along the tokens; every clip holds 1 to 1500 tokens, and one holds exactly 1500.
All inputs are finite; a program needn't handle non-finite values.
Results may differ from the reference program's by a relative error of at most 0.0003.
Values sent between devices are 32-bit elements; how exact they have to be, the bound alone decides.
A program may use at most 192 MiB of HBM per device.

```python
import math
import jax
import jax.numpy as jnp
import numpy as np
from jax import lax

D = 768
HEADS = 12
HEAD_DIM = 64
FF = 3072
TOK_DEV = 512
MOST = 1500
REACH = 3
TOKENS = 8192
CLIPS = 9
N_DP = 16


def draw_input_weight(key, part):
    first, second, third = jax.random.split(jax.random.fold_in(key, 7), 3)
    base_scale = D ** (-0.5)
    query_part = jax.random.normal(first, (D, D), jnp.float32) * base_scale
    key_part = jax.random.normal(second, (D, D), jnp.float32) * base_scale
    value_part = jax.random.normal(third, (D, D), jnp.float32) * base_scale
    stacked = jnp.stack([query_part, key_part, value_part], axis=1)
    return jnp.clip(stacked, -1.5, 1.5)


def block_scale(own_key, extent, pieces, smallest, largest):
    def one(position, parts):
        steps = jax.random.uniform(jax.random.fold_in(jax.random.fold_in(own_key, 6), position), (parts,), jnp.float32, smallest / len(pieces), largest / len(pieces))
        return jnp.repeat(jnp.exp(steps), extent[position] // parts).reshape((-1,) + (1,) * (len(extent) - position - 1))

    level = one(*pieces[0])
    for cut in pieces[1:]:
        level = level * one(*cut)
    return level


def split_up(number_of, total, bound, slope):
    loads = [(1 << 20) // math.isqrt(standing ** slope) + 1 for standing in range(2, number_of + 1)]
    spare, given = total - bound - (number_of - 1), [1] * (number_of - 1)
    while spare > 0:
        movable = [i for i in range(number_of - 1) if given[i] < bound]
        mass, left = sum([loads[i] for i in movable]), spare
        for i in movable:
            more = min(bound - given[i], max(1, left * loads[i] // mass), spare)
            given[i] = given[i] + more
            spare = spare - more
    return np.array([bound] + given)


def uneven(rng, count, total, limit, skew):
    if count == 2:
        one = jax.random.randint(rng, (), max(1, total - limit), min(limit, total - 1) + 1)
        return jnp.stack([one, total - one])
    tallies = jnp.asarray(split_up(count, total, limit, skew), jnp.int32)
    twos = (count - 1) // 2
    giver, taker = tallies[1:1 + 2 * twos:2], tallies[2:2 + 2 * twos:2]
    room = jnp.minimum(giver - 1, limit - taker)
    shifted = jax.random.randint(jax.random.fold_in(rng, 1), (twos,), 0, 1 << 20) % (room + 1)
    tallies = tallies.at[1:1 + 2 * twos:2].set(giver - shifted).at[2:2 + 2 * twos:2].set(taker + shifted)
    return tallies[jax.random.permutation(jax.random.fold_in(rng, 2), count)]


def scatter_about(rng, dims, scale, bound, shards=(), held_as=jnp.bfloat16):
    drawn = scale * jax.random.normal(rng, dims, jnp.float32)
    if shards:
        drawn = drawn * block_scale(rng, dims, shards, -0.22, 0.18)
    return jnp.clip(drawn, -bound, bound).astype(held_as)


def setup_inputs(seed: int = 0) -> dict:
    arg_keys = jax.random.split(jax.random.key(seed), 16)
    frames = scatter_about(arg_keys[0], (TOKENS, D), 1.0, 6.0, ((0, 16),), jnp.float32)
    clip_ids = jnp.searchsorted(jnp.cumsum(uneven(arg_keys[1], CLIPS, TOKENS, MOST, 1)), jnp.arange(TOKENS), side="right").astype(jnp.int32)
    first_gain = jnp.clip(1.0 + 0.1 * jax.random.normal(arg_keys[2], (D,), jnp.float32), 0.5, 1.5)
    first_shift = scatter_about(arg_keys[3], (D,), 0.3, 1.75, (), jnp.float32)
    input_weight = draw_input_weight(jax.random.fold_in(arg_keys[15], 71), 0)
    input_bias = scatter_about(arg_keys[5], (2, D), 0.3, 1.75, ((1, 2),), jnp.float32)
    output_weight = scatter_about(arg_keys[6], (D, D), (D // 32) ** -0.5, 1.25, ((0, 2),), jnp.float32)
    output_bias = scatter_about(arg_keys[7], (D,), 0.3, 1.75, (), jnp.float32)
    second_gain = jnp.clip(1.0 + 0.1 * jax.random.normal(arg_keys[8], (D,), jnp.float32), 0.5, 1.5)
    second_shift = scatter_about(arg_keys[9], (D,), 0.3, 1.75, (), jnp.float32)
    expand_weight = scatter_about(arg_keys[10], (D, FF), D ** -0.5, 0.21875, ((1, 2),), jnp.float32)
    expand_bias = scatter_about(arg_keys[11], (FF,), 0.5, 3.0, ((0, 2),), jnp.float32)
    contract_weight = scatter_about(arg_keys[12], (FF, D), FF ** -0.5, 0.109375, ((0, 2),), jnp.float32)
    contract_bias = scatter_about(arg_keys[13], (D,), 0.3, 1.75, (), jnp.float32)
    cotangent = scatter_about(arg_keys[14], (TOKENS, D), 1.0, 6.0, ((0, 16),), jnp.float32)
    return {"frames": frames, "clip_ids": clip_ids, "first_gain": first_gain, "first_shift": first_shift, "input_weight": input_weight, "input_bias": input_bias, "output_weight": output_weight, "output_bias": output_bias, "second_gain": second_gain, "second_shift": second_shift, "expand_weight": expand_weight, "expand_bias": expand_bias, "contract_weight": contract_weight, "contract_bias": contract_bias, "cotangent": cotangent}


epsilon = 1e-05
highest = lax.Precision.HIGHEST

def layer_norm(matrix_rows, gain, shift):
    average = lax.optimization_barrier(jnp.mean(matrix_rows, axis=-1, keepdims=True))
    centered = matrix_rows - average
    spread = lax.optimization_barrier(jnp.mean(centered * centered, axis=-1, keepdims=True))
    return centered * lax.rsqrt(spread + epsilon) * gain + shift

def attention(queries, keys, values, clip_ids):
    padding = REACH * TOK_DEV
    window_rows = (2 * REACH + 1) * TOK_DEV
    keys_padded = jnp.pad(keys, ((padding, padding), (0, 0)))
    values_padded = jnp.pad(values, ((padding, padding), (0, 0)))
    ids_padded = jnp.pad(clip_ids, (padding, padding), constant_values=-1)
    score_scale = HEAD_DIM ** (-0.5)

    def one_block(block_index):
        start = (block_index * TOK_DEV).astype(jnp.int32)
        block_queries = lax.dynamic_slice_in_dim(queries, start, TOK_DEV, 0).reshape(TOK_DEV, HEADS, HEAD_DIM)
        block_keys = lax.dynamic_slice_in_dim(keys_padded, start, window_rows, 0).reshape(window_rows, HEADS, HEAD_DIM)
        block_values = lax.dynamic_slice_in_dim(values_padded, start, window_rows, 0).reshape(window_rows, HEADS, HEAD_DIM)
        query_ids = lax.dynamic_slice_in_dim(clip_ids, start, TOK_DEV, 0)
        key_ids = lax.dynamic_slice_in_dim(ids_padded, start, window_rows, 0)
        scores = jnp.einsum('qhd,khd->hqk', block_queries, block_keys, precision=highest) * score_scale
        same_clip = query_ids[:, None] == key_ids[None, :]
        scores = jnp.where(same_clip[None], scores, -1e+30)
        weights = jax.nn.softmax(scores, axis=-1)
        attended = jnp.einsum('hqk,khd->qhd', weights, block_values, precision=highest)
        return attended.reshape(TOK_DEV, HEADS * HEAD_DIM)
    blocks = lax.map(jax.checkpoint(one_block), jnp.arange(N_DP, dtype=jnp.int32))
    return blocks.reshape(TOKENS, HEADS * HEAD_DIM)

def reference(frames, clip_ids, first_gain, first_shift, input_weight, input_bias, output_weight, output_bias, second_gain, second_shift, expand_weight, expand_bias, contract_weight, contract_bias, cotangent):

    def forward(frames_in, first_gain, first_shift, input_weight, input_bias, output_weight, output_bias, second_gain, second_shift, expand_weight, expand_bias, contract_weight, contract_bias):
        first_normed = layer_norm(frames_in, first_gain, first_shift)
        queries = jnp.dot(first_normed, input_weight[:, 0, :], precision=highest, preferred_element_type=jnp.float32) + input_bias[0]
        keys = jnp.dot(first_normed, input_weight[:, 1, :], precision=highest, preferred_element_type=jnp.float32)
        values = jnp.dot(first_normed, input_weight[:, 2, :], precision=highest, preferred_element_type=jnp.float32) + input_bias[1]
        attended = attention(queries, keys, values, clip_ids)
        residual = frames_in + jnp.dot(attended, output_weight, precision=highest, preferred_element_type=jnp.float32) + output_bias
        second_normed = layer_norm(residual, second_gain, second_shift)
        pre_active = jnp.dot(second_normed, expand_weight, precision=highest, preferred_element_type=jnp.float32) + expand_bias
        activated = jax.nn.gelu(pre_active, approximate=False)
        return residual + jnp.dot(activated, contract_weight, precision=highest, preferred_element_type=jnp.float32) + contract_bias
    block_output, pullback = jax.vjp(forward, frames, first_gain, first_shift, input_weight, input_bias, output_weight, output_bias, second_gain, second_shift, expand_weight, expand_bias, contract_weight, contract_bias)
    grad_frames, grad_first_gain, grad_first_shift, grad_input_weight, grad_input_bias, grad_output_weight, grad_output_bias, grad_second_gain, grad_second_shift, grad_expand_weight, grad_expand_bias, grad_contract_weight, grad_contract_bias = pullback(cotangent)
    return (block_output, grad_frames, grad_first_gain, grad_first_shift, grad_input_weight, grad_input_bias, grad_output_weight, grad_output_bias, grad_second_gain, grad_second_shift, grad_expand_weight, grad_expand_bias, grad_contract_weight, grad_contract_bias)
```

```python
import functools
import math

import jax
import jax.numpy as jnp
from jax import lax
from jax.experimental import pallas as pl
from jax.experimental.pallas import tpu as pltpu
from jax.sharding import PartitionSpec as P

HEAD_DIM = 64
REACH = 3
PAIR = 2 * HEAD_DIM
TILE = 256
LOG2E = math.log2(math.e)
VMEM_LIMIT = 60 * 1024 * 1024

epsilon = 1e-05
high = lax.Precision.HIGH
f32 = jnp.float32
bf16 = jnp.bfloat16


def contract(left, right, left_dim, right_dim):
    return lax.dot_general(
        left,
        right,
        (((left_dim,), (right_dim,)), ((), ())),
        precision=high,
        preferred_element_type=f32,
    )


def normalize(rows):
    average = jnp.mean(rows, axis=1, keepdims=True)
    centered = rows - average
    scaled = lax.rsqrt(jnp.mean(centered * centered, axis=1, keepdims=True) + epsilon)
    return centered * scaled, scaled


def norm_backward(grad_normed, standard, scaled, gain):
    grad_standard = grad_normed * gain
    return scaled * (
        grad_standard
        - jnp.mean(grad_standard, axis=1, keepdims=True)
        - standard * jnp.mean(grad_standard * standard, axis=1, keepdims=True)
    )


def gelu_parts(pre_active):
    cumulative = 0.5 * (1.0 + jax.scipy.special.erf(pre_active * 0.7071067811865476))
    density = jnp.exp(-0.5 * pre_active * pre_active) * 0.3989422804014327
    return pre_active * cumulative, cumulative + pre_active * density


def split(x):
    top = x.astype(bf16)
    return top, (x - top.astype(f32)).astype(bf16)


def mxu(left, right):
    return jnp.dot(left, right, preferred_element_type=f32)


def head_parts(x):
    top = x.astype(bf16).astype(f32)
    low = x - top
    top_turned = pltpu.roll(top, HEAD_DIM, 1)
    low_turned = pltpu.roll(low, HEAD_DIM, 1)
    first = lax.broadcasted_iota(jnp.int32, x.shape, 1) < HEAD_DIM
    return (
        jnp.where(first, top, low_turned).astype(bf16),
        jnp.where(first, top_turned, low).astype(bf16),
    )


def head_parts_columns(x):
    top, low = split(x)
    return (
        jnp.concatenate([top[:HEAD_DIM], low[:HEAD_DIM]], axis=0),
        jnp.concatenate([top[HEAD_DIM:], low[HEAD_DIM:]], axis=0),
    )


def doubled(parts, axis):
    top, low = (
        (parts[:HEAD_DIM], parts[HEAD_DIM:]) if axis == 0 else (parts[:, :HEAD_DIM], parts[:, HEAD_DIM:])
    )
    return jnp.concatenate([top, top, low, low], axis=axis)


def twice(parts, axis):
    return jnp.concatenate([parts, parts], axis=axis)


def same_clip(key_ids, query_ids):
    lanes = query_ids.shape[1] // PAIR
    return jnp.concatenate([key_ids] * lanes, axis=1) == query_ids


def tile_range(bounds):
    n = bounds.shape[0]
    low, high_ = bounds[0, 0], bounds[0, 1]
    for i in range(1, n):
        low = jnp.minimum(low, bounds[i, 0])
        high_ = jnp.maximum(high_, bounds[i, 1])
    return low, high_


def attend_kernel(bounds, q_ref, k_ref, v_ref, kid_ref, qid_ref, o_ref, lse_ref, kc, vc):
    tokens = q_ref.shape[0]

    def prepare(j, carry):
        rows = pl.ds(pl.multiple_of(j * TILE, TILE), TILE)
        a, b = head_parts(k_ref[rows, :])
        kc[0, rows, :] = a
        kc[1, rows, :] = b
        a, b = head_parts_columns(v_ref[rows, :].T)
        vc[0, j] = a
        vc[1, j] = b
        return carry

    lax.fori_loop(*tile_range(bounds), prepare, 0)
    for i in range(tokens // TILE):
        columns = slice(i * TILE, (i + 1) * TILE)
        query_ids = qid_ref[:, columns]
        q = [doubled(part, 0) for part in head_parts_columns(q_ref[columns, :].T)]

        def step(j, carry, q=q, query_ids=query_ids):
            rows = pl.ds(pl.multiple_of(j * TILE, TILE), TILE)
            valid = same_clip(kid_ref[rows, :], query_ids)
            out = []
            for e in range(2):
                top, total, acc = carry[3 * e : 3 * e + 3]
                s = jnp.where(valid, mxu(twice(kc[e, rows, :], 1), q[e]), -1e30)
                new_top = jnp.maximum(top, jnp.max(s, axis=0, keepdims=True))
                fade = jnp.exp2(top - new_top)
                p = jnp.exp2(s - new_top)
                total = total * fade + jnp.sum(p, axis=0, keepdims=True)
                p_top, p_low = split(p)
                v = vc[e, j]
                acc = acc * fade + mxu(v, p_top) + mxu(v, p_low)
                out += [new_top, total, acc]
            return tuple(out)

        start = (
            jnp.full((1, TILE), -1e30, f32),
            jnp.zeros((1, TILE), f32),
            jnp.zeros((PAIR, TILE), f32),
        )
        result = lax.fori_loop(bounds[i, 0], bounds[i, 1], step, start * 2)
        for e in range(2):
            top, total, acc = result[3 * e : 3 * e + 3]
            o_ref[e * HEAD_DIM : (e + 1) * HEAD_DIM, columns] = (
                acc[:HEAD_DIM] + acc[HEAD_DIM:]
            ) / total
            lse_ref[0, e : e + 1, columns] = top + jnp.log2(total)


def query_grad_kernel(
    bounds, q_ref, k_ref, v_ref, do_ref, lse_ref, inner_ref, kid_ref, qid_ref, dq_ref, kc, vc, kt
):
    tokens = q_ref.shape[0]

    def prepare(j, carry):
        rows = pl.ds(pl.multiple_of(j * TILE, TILE), TILE)
        k = k_ref[rows, :]
        kc[0, rows, :], kc[1, rows, :] = head_parts(k)
        vc[0, rows, :], vc[1, rows, :] = head_parts(v_ref[rows, :])
        kt[0, j], kt[1, j] = head_parts_columns(k.T)
        return carry

    lax.fori_loop(*tile_range(bounds), prepare, 0)
    for i in range(tokens // TILE):
        columns = slice(i * TILE, (i + 1) * TILE)
        query_ids = qid_ref[:, columns]
        q = [doubled(part, 0) for part in head_parts_columns(q_ref[columns, :].T)]
        do = [doubled(part, 0) for part in head_parts_columns(do_ref[:, columns])]

        def step(j, carry, q=q, do=do, query_ids=query_ids, columns=columns):
            rows = pl.ds(pl.multiple_of(j * TILE, TILE), TILE)
            valid = same_clip(kid_ref[rows, :], query_ids)
            out = []
            for e in range(2):
                s = mxu(twice(kc[e, rows, :], 1), q[e])
                p = jnp.where(valid, jnp.exp2(s - lse_ref[0, e : e + 1, columns]), 0.0)
                dp = mxu(twice(vc[e, rows, :], 1), do[e])
                ds_top, ds_low = split(p * (dp - inner_ref[0, e : e + 1, columns]))
                k = kt[e, j]
                out.append(carry[e] + mxu(k, ds_top) + mxu(k, ds_low))
            return tuple(out)

        zero = jnp.zeros((PAIR, TILE), f32)
        result = lax.fori_loop(bounds[i, 0], bounds[i, 1], step, (zero, zero))
        for e in range(2):
            dq_ref[e * HEAD_DIM : (e + 1) * HEAD_DIM, columns] = (
                result[e][:HEAD_DIM] + result[e][HEAD_DIM:]
            ) * (HEAD_DIM ** (-0.5))


def key_grad_kernel(
    bounds,
    q_ref,
    k_ref,
    v_ref,
    do_ref,
    lse_ref,
    inner_ref,
    kid_ref,
    qid_ref,
    dk_ref,
    dv_ref,
    qc,
    doc,
    qt,
    dot,
):
    tokens = k_ref.shape[0]

    def prepare(j, carry):
        rows = pl.ds(pl.multiple_of(j * TILE, TILE), TILE)
        q = q_ref[rows, :]
        do = do_ref[rows, :]
        qc[0, rows, :], qc[1, rows, :] = head_parts(q)
        doc[0, rows, :], doc[1, rows, :] = head_parts(do)
        qt[0, j], qt[1, j] = head_parts_columns(q.T)
        dot[0, j], dot[1, j] = head_parts_columns(do.T)
        return carry

    lax.fori_loop(*tile_range(bounds), prepare, 0)
    for i in range(tokens // TILE):
        own = slice(i * TILE, (i + 1) * TILE)
        key_ids = kid_ref[own, :]
        k = [doubled(part, 1) for part in head_parts(k_ref[own, :])]
        v = [doubled(part, 1) for part in head_parts(v_ref[own, :])]

        def step(j, carry, k=k, v=v, key_ids=key_ids):
            rows = pl.ds(pl.multiple_of(j * TILE, TILE), TILE)
            valid = same_clip(key_ids, qid_ref[pl.ds(j, 1), :])
            out = []
            for e in range(2):
                dk, dv = carry[2 * e : 2 * e + 2]
                s = mxu(k[e], twice(qt[e, j], 0))
                p = jnp.where(valid, jnp.exp2(s - lse_ref[0, e, pl.ds(j, 1), :]), 0.0)
                dp = mxu(v[e], twice(dot[e, j], 0))
                p_top, p_low = split(p)
                ds_top, ds_low = split(p * (dp - inner_ref[0, e, pl.ds(j, 1), :]))
                do = doc[e, rows, :]
                q = qc[e, rows, :]
                dv = dv + mxu(p_top, do) + mxu(p_low, do)
                dk = dk + mxu(ds_top, q) + mxu(ds_low, q)
                out += [dk, dv]
            return tuple(out)

        zero = jnp.zeros((TILE, PAIR), f32)
        result = lax.fori_loop(bounds[i, 0], bounds[i, 1], step, (zero,) * 4)
        first = lax.broadcasted_iota(jnp.int32, (TILE, PAIR), 1) < HEAD_DIM
        for ref, at, scale in ((dk_ref, 0, math.log(2.0)), (dv_ref, 1, 1.0)):
            whole = [x + pltpu.roll(x, HEAD_DIM, 1) for x in (result[at], result[2 + at])]
            ref[own, :] = jnp.where(first, whole[0], whole[1]) * scale


def pair_rows(rows, column=0, row=0):
    return pl.BlockSpec((rows, PAIR), lambda p, *_: (row, column + p))


def pair_columns(columns):
    return pl.BlockSpec((PAIR, columns), lambda p, *_: (p, 0))


def pair_block(*shape):
    zeros = (0,) * len(shape)
    return pl.BlockSpec((1, *shape), lambda p, *_: (p, *zeros))


def whole_block(*shape):
    zeros = (0,) * len(shape)
    return pl.BlockSpec(shape, lambda p, *_: zeros)


def attention_call(kernel, pairs, in_specs, out_specs, out_shape, scratch, flops, args):
    return pl.pallas_call(
        kernel,
        out_shape=out_shape,
        grid_spec=pltpu.PrefetchScalarGridSpec(
            num_scalar_prefetch=1,
            grid=(pairs,),
            in_specs=in_specs,
            out_specs=out_specs,
            scratch_shapes=scratch,
        ),
        compiler_params=pltpu.CompilerParams(vmem_limit_bytes=VMEM_LIMIT),
        cost_estimate=pl.CostEstimate(flops=flops, bytes_accessed=20_000_000, transcendentals=0),
    )(*args)


def attend(bounds, qkv, key_ids, query_ids):
    window, width = qkv.shape[0], qkv.shape[1] // 3
    tokens = query_ids.shape[1]
    pairs = width // PAIR
    return attention_call(
        attend_kernel,
        pairs,
        [
            pair_rows(tokens, 0, REACH),
            pair_rows(window, pairs),
            pair_rows(window, 2 * pairs),
            whole_block(window, PAIR),
            whole_block(1, tokens),
        ],
        [pair_columns(tokens), pair_block(2, tokens)],
        [
            jax.ShapeDtypeStruct((width, tokens), f32),
            jax.ShapeDtypeStruct((pairs, 2, tokens), f32),
        ],
        [
            pltpu.VMEM((2, window, PAIR), bf16),
            pltpu.VMEM((2, window // TILE, PAIR, TILE), bf16),
        ],
        20_000_000_000,
        (bounds, qkv, qkv, qkv, key_ids, query_ids),
    )


def query_grad(bounds, qkv, do, lse, inner, key_ids, query_ids):
    width, tokens = do.shape
    window = qkv.shape[0]
    pairs = width // PAIR
    return attention_call(
        query_grad_kernel,
        pairs,
        [
            pair_rows(tokens, 0, REACH),
            pair_rows(window, pairs),
            pair_rows(window, 2 * pairs),
            pair_columns(tokens),
            pair_block(2, tokens),
            pair_block(2, tokens),
            whole_block(window, PAIR),
            whole_block(1, tokens),
        ],
        pair_columns(tokens),
        jax.ShapeDtypeStruct((width, tokens), f32),
        [
            pltpu.VMEM((2, window, PAIR), bf16),
            pltpu.VMEM((2, window, PAIR), bf16),
            pltpu.VMEM((2, window // TILE, PAIR, TILE), bf16),
        ],
        30_000_000_000,
        (bounds, qkv, qkv, qkv, do, lse, inner, key_ids, query_ids),
    )


def key_grad(bounds, qkv, do, lse, inner, key_ids, query_ids):
    window, width = do.shape
    tokens = key_ids.shape[0]
    tiles = window // TILE
    pairs = width // PAIR
    return attention_call(
        key_grad_kernel,
        pairs,
        [
            pair_rows(window),
            pair_rows(tokens, pairs, REACH),
            pair_rows(tokens, 2 * pairs, REACH),
            pair_rows(window),
            pair_block(2, tiles, TILE),
            pair_block(2, tiles, TILE),
            whole_block(tokens, PAIR),
            whole_block(tiles, TILE),
        ],
        [pair_rows(tokens), pair_rows(tokens)],
        [jax.ShapeDtypeStruct((tokens, width), f32)] * 2,
        [
            pltpu.VMEM((2, window, PAIR), bf16),
            pltpu.VMEM((2, window, PAIR), bf16),
            pltpu.VMEM((2, tiles, PAIR, TILE), bf16),
            pltpu.VMEM((2, tiles, PAIR, TILE), bf16),
        ],
        40_000_000_000,
        (bounds, qkv, qkv, qkv, do, lse, inner, key_ids, query_ids),
    )


def halo_kernel(
    norm,
    extra,
    block_ref,
    weight_ref,
    bias_ref,
    scale_ref,
    gain_ref,
    shift_ref,
    out_ref,
    *rest,
):
    rest = list(rest)
    extra_ref = rest.pop(0) if extra else None
    mine, other, result, w_top, w_low, load_sem, send_sem, recv_sem = rest[:8]
    swap_send, swap_recv, store_sem, extra_sem = rest[8:]
    me = lax.axis_index("dp")
    core = lax.axis_index("mp")
    n_dp = lax.axis_size("dp")
    half = other.shape[1]
    sends = 2 * REACH

    def offset_of(k):
        return (k // 2 + 1) * (1 - 2 * (k % 2))

    def within(k):
        return jnp.logical_and(me + k >= 0, me + k < n_dp)

    def load():
        return pltpu.make_async_copy(block_ref, mine.at[0], load_sem.at[0])

    def send(k):
        return pltpu.make_async_remote_copy(
            src_ref=mine.at[0],
            dst_ref=mine.at[k + 1],
            send_sem=send_sem.at[k],
            recv_sem=recv_sem.at[k],
            device_id={"dp": me + offset_of(k)},
            device_id_type=pl.DeviceIdType.MESH,
        )

    def swap(t):
        return pltpu.make_async_remote_copy(
            src_ref=mine.at[t, pl.ds(0, half)],
            dst_ref=other.at[t],
            send_sem=swap_send.at[t],
            recv_sem=swap_recv.at[t],
            device_id={"mp": 1 - core},
            device_id_type=pl.DeviceIdType.MESH,
        )

    def rows_of(t, which):
        piece = jnp.where(t == 0, REACH, REACH - offset_of(t - 1))
        return pl.ds(pl.multiple_of((2 * piece + which) * half, half), half)

    def store(t, which):
        rows = rows_of(t, which)
        return pltpu.make_async_copy(
            result.at[rows], out_ref.at[rows], store_sem.at[2 * t + jnp.where(which == core, 0, 1)]
        )

    def keep(t):
        return pltpu.make_async_copy(
            mine.at[t, pl.ds(half, extra)],
            extra_ref.at[jnp.where(t == 0, REACH, REACH - offset_of(t - 1))],
            extra_sem.at[t],
        )

    def project(x, t, which):
        if norm:
            average = jnp.mean(x, axis=1, keepdims=True)
            centered = x - average
            scaled = lax.rsqrt(jnp.mean(centered * centered, axis=1, keepdims=True) + epsilon)
            x = centered * scaled * gain_ref[...] + shift_ref[...]
        top, low = split(x)
        product = mxu(top, w_top[...]) + mxu(low, w_top[...]) + mxu(top, w_low[...])
        result[rows_of(t, which), :] = (product + bias_ref[...]) * scale_ref[...]
        store(t, which).start()

    load().start()
    barrier = pltpu.get_barrier_semaphore()
    pl.semaphore_signal(
        barrier, inc=1, device_id={"mp": 1 - core}, device_id_type=pl.DeviceIdType.MESH
    )
    for k in range(sends):

        @pl.when(within(offset_of(k)))
        def _(k=k):
            pl.semaphore_signal(
                barrier,
                inc=1,
                device_id={"dp": me + offset_of(k)},
                device_id_type=pl.DeviceIdType.MESH,
            )

    peers = 1
    for k in range(sends):
        peers = peers + within(offset_of(k)).astype(jnp.int32)
    pl.semaphore_wait(barrier, peers)

    load().wait()
    for k in range(sends):

        @pl.when(within(offset_of(k)))
        def _(k=k):
            send(k).start()

    if len(weight_ref.shape) == 3:
        each = weight_ref.shape[2]
        for i in range(weight_ref.shape[1]):
            columns = slice(i * each, (i + 1) * each)
            w_top[:, columns], w_low[:, columns] = split(weight_ref[:, i, :])
    else:
        w_top[...], w_low[...] = split(weight_ref[...])

    def step(t, carry):
        @pl.when(jnp.logical_and(t >= 1, t <= sends))
        def _():
            @pl.when(within(-offset_of(t - 1)))
            def _():
                send(t - 1).wait_recv()

        @pl.when(jnp.logical_and(t <= sends, jnp.logical_or(t == 0, within(-offset_of(t - 1)))))
        def _():
            swap(t).start()
            if extra:
                keep(t).start()
            project(mine[t, pl.ds(0, half), :], t, core)

        last = t - 1

        @pl.when(jnp.logical_and(t >= 1, jnp.logical_or(last == 0, within(-offset_of(last - 1)))))
        def _():
            swap(last).wait()
            project(other[last], last, 1 - core)

        return carry

    lax.fori_loop(0, sends + 2, step, 0)
    for t in range(sends + 1):

        def finish(t=t):
            store(t, core).wait()
            store(t, 1 - core).wait()
            if extra:
                keep(t).wait()

        if t == 0:
            finish()
        else:
            pl.when(within(-offset_of(t - 1)))(finish)
            pl.when(within(offset_of(t - 1)))(lambda t=t: send(t - 1).wait_send())


def halo_project(block, weight, bias, scale, collective_id, gain=None, shift=None, extra=0):
    half, width = block.shape[0] - extra, block.shape[1]
    columns = math.prod(weight.shape[1:])
    pieces = 2 * REACH + 1
    norm = gain is not None
    if not norm:
        gain = shift = jnp.zeros((width,), f32)
    window = pieces * 2 * half
    any_space = pl.BlockSpec(memory_space=pl.ANY)
    vmem = pl.BlockSpec(memory_space=pltpu.VMEM)
    out_shape = [jax.ShapeDtypeStruct((window, columns), f32)]
    if extra:
        out_shape.append(jax.ShapeDtypeStruct((pieces, extra, width), f32))
    return pl.pallas_call(
        functools.partial(halo_kernel, norm, extra),
        out_shape=out_shape,
        in_specs=[any_space, vmem, vmem, vmem, vmem, vmem],
        out_specs=[any_space] * len(out_shape),
        scratch_shapes=[
            pltpu.VMEM((pieces, half + extra, width), f32),
            pltpu.VMEM((pieces, half, width), f32),
            pltpu.VMEM((window, columns), f32),
            pltpu.VMEM((width, columns), bf16),
            pltpu.VMEM((width, columns), bf16),
            pltpu.SemaphoreType.DMA((1,)),
            pltpu.SemaphoreType.DMA((2 * REACH,)),
            pltpu.SemaphoreType.DMA((2 * REACH,)),
            pltpu.SemaphoreType.DMA((pieces,)),
            pltpu.SemaphoreType.DMA((pieces,)),
            pltpu.SemaphoreType.DMA((2 * pieces,)),
            pltpu.SemaphoreType.DMA((pieces,)),
        ],
        compiler_params=pltpu.CompilerParams(
            collective_id=collective_id, has_side_effects=True, vmem_limit_bytes=VMEM_LIMIT
        ),
        cost_estimate=pl.CostEstimate(
            flops=80_000_000_000, bytes_accessed=20_000_000, transcendentals=0
        ),
    )(block, weight, bias[None, :], scale[None, :], gain[None, :], shift[None, :])


def stream_plan(n_dp, rows):
    levels = n_dp.bit_length() - 1
    unit = 8 * n_dp
    orders = [(0, 2, 1), (1, 2, 0), (2, 0, 1), (0, 1, 2), (1, 0, 2), (2, 1, 0)] * 2
    units = max(-(-rows // unit), len(orders))
    plan, base = [], 0
    for i, head in enumerate(orders):
        order = [b for b in head if b < levels] + list(range(3, levels))
        size = unit * ((units + i) // len(orders))
        plan.append((order, base, size))
        base += size
    return plan, base


def sum_kernel(plan, layout, *refs):
    n_parts = len(layout)
    x_refs, o_refs = refs[:n_parts], refs[n_parts : 2 * n_parts]
    total, arrived, whole, load_sem, store_sem, send_sem, recv_sem = refs[2 * n_parts :]
    width = total.shape[1]
    me = lax.axis_index("dp")
    levels = len(plan[0][0])
    values = [(me // (1 << b)) % 2 for b in range(levels)]
    partners = [me + (1 - 2 * values[b]) * (1 << b) for b in range(levels)]
    barrier = pltpu.get_barrier_semaphore()
    loads, stores, at = [], [], 0
    for i, (rows, cuts) in enumerate(layout):
        for c in range(cuts):
            columns = pl.ds(c * width, width)
            held = pl.ds(at, rows)
            sem = len(loads)
            loads.append(
                pltpu.make_async_copy(x_refs[i].at[:, columns], total.at[held], load_sem.at[sem])
            )
            stores.append(
                pltpu.make_async_copy(whole.at[held], o_refs[i].at[:, columns], store_sem.at[sem])
            )
            at += rows
    for load in loads:
        load.start()
    for partner in partners:
        pl.semaphore_signal(
            barrier, inc=1, device_id={"dp": partner}, device_id_type=pl.DeviceIdType.MESH
        )
    pl.semaphore_wait(barrier, levels)

    slots, at = [], 0
    for order, _, size in plan:
        slots.append([])
        for k in range(levels):
            slots[-1].append((at, size >> (k + 1)))
            at += size >> (k + 1)
    starts = []
    for order, base, size in plan:
        rows = [base]
        for k, b in enumerate(order):
            rows.append(rows[-1] + values[b] * (size >> (k + 1)))
        starts.append(rows)

    def at_rows(start, size):
        return pl.ds(pl.multiple_of(start, 8), size)

    def copy(i, k, source, target, which):
        return pltpu.make_async_remote_copy(
            src_ref=source,
            dst_ref=target,
            send_sem=send_sem.at[i, which],
            recv_sem=recv_sem.at[i, which],
            device_id={"dp": partners[plan[i][0][k]]},
            device_id_type=pl.DeviceIdType.MESH,
        )

    def scatter(i, k):
        at, half = slots[i][k]
        away = 1 - values[plan[i][0][k]]
        source = total.at[at_rows(starts[i][k] + away * half, half)]
        return copy(i, k, source, arrived.at[pl.ds(at, half)], k)

    def gather(i, k):
        rows = whole.at[at_rows(starts[i][k + 1], slots[i][k][1])]
        return copy(i, k, rows, rows, levels + k)

    streams = range(len(plan))
    for load in loads:
        load.wait()
    for i in streams:
        scatter(i, 0).start()
    for k in range(levels):
        for i in streams:
            scatter(i, k).wait()
            at, half = slots[i][k]
            kept = at_rows(starts[i][k + 1], half)
            added = total[kept, :] + arrived[pl.ds(at, half), :]
            if k + 1 < levels:
                total[kept, :] = added
                scatter(i, k + 1).start()
            else:
                whole[kept, :] = added
                gather(i, k).start()
    for k in reversed(range(levels)):
        for i in streams:
            gather(i, k).wait()
            if k > 0:
                gather(i, k - 1).start()
    for store in stores:
        store.start()
    for store in stores:
        store.wait()


def stream_sum(parts, width, n_dp):
    layout = [(part.shape[0], part.shape[1] // width) for part in parts]
    rows = sum(height * cuts for height, cuts in layout)
    plan, padded = stream_plan(n_dp, rows)
    if padded > rows:
        parts = [*parts, jnp.zeros((padded - rows, width), f32)]
        layout.append((padded - rows, 1))
    copies = sum(cuts for _, cuts in layout)
    slot_rows = sum(size - (size >> len(order)) for order, _, size in plan)
    levels = len(plan[0][0])
    any_space = pl.BlockSpec(memory_space=pl.ANY)
    return pl.pallas_call(
        functools.partial(sum_kernel, plan, layout),
        out_shape=[jax.ShapeDtypeStruct(part.shape, f32) for part in parts],
        in_specs=[any_space] * len(parts),
        out_specs=[any_space] * len(parts),
        scratch_shapes=[
            pltpu.VMEM((padded, width), f32),
            pltpu.VMEM((slot_rows, width), f32),
            pltpu.VMEM((padded, width), f32),
            pltpu.SemaphoreType.DMA((copies,)),
            pltpu.SemaphoreType.DMA((copies,)),
            pltpu.SemaphoreType.DMA((len(plan), 2 * levels)),
            pltpu.SemaphoreType.DMA((len(plan), 2 * levels)),
        ],
        compiler_params=pltpu.CompilerParams(
            collective_id=0, has_side_effects=True, vmem_limit_bytes=VMEM_LIMIT
        ),
        cost_estimate=pl.CostEstimate(
            flops=80_000_000_000, bytes_accessed=20_000_000, transcendentals=0
        ),
    )(*parts)


def local(
    frames,
    clip_ids,
    first_gain,
    first_shift,
    input_weight,
    input_bias,
    output_weight,
    output_bias,
    second_gain,
    second_shift,
    expand_weight,
    expand_bias,
    contract_weight,
    contract_bias,
    cotangent,
):
    tokens, model_width = frames.shape
    local_width = input_weight.shape[2]
    pairs = local_width // PAIR
    half = tokens // 2
    window_rows = (2 * REACH + 1) * tokens
    tiles = window_rows // TILE
    device = lax.axis_index("dp")
    core = lax.axis_index("mp")
    n_dp = lax.axis_size("dp")

    def swapped(block):
        return lax.ppermute(block, "mp", [(0, 1), (1, 0)])

    def my_half(rows):
        return lax.dynamic_slice_in_dim(rows, core * half, half, 0)

    def reduced_half(partial):
        theirs = lax.dynamic_slice_in_dim(partial, (1 - core) * half, half, 0)
        return my_half(partial) + swapped(theirs)

    def both_halves(mine):
        other = swapped(mine)
        return jnp.concatenate(
            [jnp.where(core == 0, mine, other), jnp.where(core == 0, other, mine)], axis=0
        )

    padded_ids = jnp.concatenate(
        [
            jnp.full((REACH * tokens,), -1, jnp.int32),
            clip_ids,
            jnp.full((REACH * tokens,), 1 << 30, jnp.int32),
        ]
    )
    window_ids = lax.dynamic_slice_in_dim(padded_ids, device * tokens, window_rows, 0)
    own_ids = lax.dynamic_slice_in_dim(clip_ids, device * tokens, tokens, 0)
    tile_ids = own_ids.reshape(tokens // TILE, TILE)
    first_key = jnp.sum(window_ids[None, :] < tile_ids[:, :1], axis=1, dtype=jnp.int32)
    last_key = jnp.sum(window_ids[None, :] <= tile_ids[:, -1:], axis=1, dtype=jnp.int32)
    bounds = jnp.stack([first_key // TILE, (last_key + TILE - 1) // TILE], axis=1)
    key_ids = jnp.broadcast_to(window_ids[:, None], (window_rows, PAIR))
    own_key_ids = jnp.broadcast_to(own_ids[:, None], (tokens, PAIR))

    frames_half = my_half(frames)
    query_weight = input_weight[:, 0, :]
    query_scale = LOG2E * HEAD_DIM ** (-0.5)
    flat_weight = input_weight.reshape(model_width, 3 * local_width)
    no_bias = jnp.zeros((local_width,), f32)
    ones = jnp.ones((local_width,), f32)
    (projected,) = halo_project(
        frames_half,
        input_weight,
        jnp.concatenate([input_bias[0], no_bias, input_bias[1]]),
        jnp.concatenate([ones * query_scale, ones, ones]),
        1,
        first_gain,
        first_shift,
    )
    attended_columns, log_totals = attend(bounds, projected, key_ids, own_ids[None, :])

    residual_half = (
        frames_half + reduced_half(contract(attended_columns, output_weight, 0, 0)) + output_bias
    )
    second_standard, second_scaled = normalize(residual_half)
    second_normed = both_halves(second_standard * second_gain + second_shift)
    pre_active = contract(second_normed, expand_weight, 1, 0) + expand_bias
    activated, gelu_slope = gelu_parts(pre_active)
    block_half = (
        residual_half + reduced_half(contract(activated, contract_weight, 1, 0)) + contract_bias
    )
    block_output = both_halves(block_half)

    grad_pre = contract(cotangent, contract_weight, 1, 1) * gelu_slope
    grad_second = reduced_half(contract(grad_pre, expand_weight, 1, 1))
    grad_contract_weight = contract(activated, cotangent, 0, 0)
    grad_expand_weight = contract(second_normed, grad_pre, 0, 0)
    grad_expand_bias = jnp.sum(grad_pre, axis=0)
    cotangent_half = my_half(cotangent)
    grad_residual_half = cotangent_half + norm_backward(
        grad_second, second_standard, second_scaled, second_gain
    )
    grad_residual = both_halves(grad_residual_half)

    grad_attended_columns = contract(output_weight, grad_residual, 1, 1)
    inner = jnp.sum(
        (attended_columns * grad_attended_columns).reshape(pairs, 2, HEAD_DIM, tokens), axis=2
    )
    statistics = jnp.concatenate([log_totals, inner]).reshape(-1, model_width)
    grad_output_weight = contract(attended_columns, grad_residual, 1, 0)
    grad_contract_weight, grad_attended_columns = lax.optimization_barrier(
        (grad_contract_weight, grad_attended_columns)
    )
    grad_contract_weight = lax.psum(grad_contract_weight, "dp")
    grad_query_columns = query_grad(
        bounds,
        projected,
        grad_attended_columns,
        log_totals,
        inner,
        key_ids,
        own_ids[None, :],
    )
    window_grad, window_statistics = halo_project(
        jnp.concatenate([grad_residual_half, statistics], axis=0),
        output_weight.T,
        no_bias,
        ones,
        2,
        extra=statistics.shape[0],
    )
    window_statistics = window_statistics.reshape(-1, 2, pairs, 2, tokens).transpose(1, 2, 3, 0, 4)
    window_statistics = window_statistics.reshape(2, pairs, 2, tiles, TILE)
    grad_keys, grad_values = key_grad(
        bounds,
        projected,
        window_grad,
        window_statistics[0],
        window_statistics[1],
        own_key_ids,
        window_ids.reshape(tiles, TILE),
    )
    first_standard, first_scaled = normalize(frames)
    first_normed = first_standard * first_gain + first_shift
    grad_first = reduced_half(
        contract(grad_query_columns, query_weight, 0, 1)
        + contract(
            jnp.concatenate([grad_keys, grad_values], axis=1), flat_weight[:, local_width:], 1, 1
        )
    )
    grad_input_parts = [
        contract(first_normed, grad_query_columns, 0, 1),
        contract(first_normed, grad_keys, 0, 0),
        contract(first_normed, grad_values, 0, 0),
    ]
    first_standard_half = my_half(first_standard)
    grad_frames = both_halves(
        grad_residual_half
        + norm_backward(grad_first, first_standard_half, my_half(first_scaled), first_gain)
    )

    shared = jnp.stack(
        [
            jnp.sum(grad_first * first_standard_half, axis=0),
            jnp.sum(grad_first, axis=0),
            jnp.sum(grad_residual_half, axis=0),
            jnp.sum(grad_second * second_standard, axis=0),
            jnp.sum(grad_second, axis=0),
            jnp.sum(cotangent_half, axis=0),
        ]
    )
    shared = shared + swapped(shared)
    own = jnp.concatenate(
        [jnp.sum(grad_query_columns, axis=1), jnp.sum(grad_values, axis=0), grad_expand_bias]
    )
    vectors = jnp.concatenate([shared.reshape(-1), own])
    vectors = jnp.pad(vectors, (0, -vectors.shape[0] % (8 * local_width)))
    summed = stream_sum(
        [
            *grad_input_parts,
            grad_output_weight,
            grad_expand_weight,
            vectors.reshape(-1, local_width),
        ],
        local_width,
        n_dp,
    )
    grad_input_weight = jnp.stack(summed[:3], axis=1)
    grad_output_weight = summed[3]
    grad_expand_weight = summed[4]
    vectors = summed[5].reshape(-1)
    shared = vectors[: 6 * model_width].reshape(6, model_width)
    own = vectors[6 * model_width : 6 * model_width + own.shape[0]]
    return (
        block_output,
        grad_frames,
        shared[0],
        shared[1],
        grad_input_weight,
        own[: 2 * local_width].reshape(2, local_width),
        grad_output_weight,
        shared[2],
        shared[3],
        shared[4],
        grad_expand_weight,
        own[2 * local_width :],
        grad_contract_weight,
        shared[5],
    )


def solution(mesh):
    in_specs = (
        P("dp", None),
        P(),
        P(),
        P(),
        P(None, None, "mp"),
        P(None, "mp"),
        P("mp", None),
        P(),
        P(),
        P(),
        P(None, "mp"),
        P("mp"),
        P("mp", None),
        P(),
        P("dp", None),
    )
    out_specs = (
        P("dp", None),
        P("dp", None),
        P(),
        P(),
        P(None, None, "mp"),
        P(None, "mp"),
        P("mp", None),
        P(),
        P(),
        P(),
        P(None, "mp"),
        P("mp"),
        P("mp", None),
        P(),
    )
    return jax.shard_map(local, mesh=mesh, in_specs=in_specs, out_specs=out_specs, check_vma=False)
```
